32 devices in a mesh: gx: 4 (over y, x), gy: 2 (over core), gz: 4 (over z).
Axes of the slice: x: 2, y: 2, z: 4, core: 2. Of those that a mesh axis runs over, the one named last changes fastest.
Arguments:
- star_residual: bfloat16 [128, 64, 1152], P(('gx', 'gy', 'gz')), may hold values from -6 to 6
- patch_inverse: bfloat16 [128, 1152, 1152], P(('gx', 'gy', 'gz')), may hold values from -0.1875 to 0.1875
- block_owner: int32 [128, 9], P(('gx', 'gy', 'gz')), may hold values from 0 to 31, as said below
- block_slot: int32 [128, 9], P(('gx', 'gy', 'gz')), may hold values from 0 to 1, as said below
- recv_target: int32 [32, 27, 2], P(('gx', 'gy', 'gz')), may hold values from -1 to 7, as said below
Outputs:
- owned_sum: float32 [256, 64, 128], P(('gx', 'gy', 'gz'))
- combined: float32 [128, 9, 64, 128], P(('gx', 'gy', 'gz'))
The draws below stay inside these ranges and needn't reach their ends.
Inputs may be any that keep to these rules, and one draw needn't show every extreme that they name: `block_owner`: each block's owner is the block's own partition or one whose coordinate differs by at most one step along each of the three mesh axes, counted with wrap-around. `block_slot`: blocks of one partition that have the same owner have distinct slots; in every partition some owner receives exactly 2 of its blocks. `recv_target`: every slot that a block uses maps to an owned block of its owner; slots that no block uses hold -1.
All inputs are finite; a program needn't handle non-finite values.
Results may differ from the reference program's by a relative error of at most 0.0003.
Values sent between devices are 32-bit elements; how exact they have to be, the bound alone decides.
A program may use at most 64 MiB of HBM per device.

```python
import jax
import jax.numpy as jnp
from jax import lax

BW = 128
PDOF = 1152
PATCH_DEV = 4
RHS = 64
OWNB = 8
CAP = 2
NBLK = 9
PX = 4
PY = 2
PZ = 4
NDEV = 32
PATCHES = 128


def axis_deltas(extent):
    if extent == 1:
        return [0]
    if extent == 2:
        return [0, 1]
    return [-1, 0, 1]


def routing(key):
    offsets = [(a, b, c) for a in axis_deltas(PX) for b in axis_deltas(PY) for c in axis_deltas(PZ)]
    offset_total = len(offsets)
    step_x = jnp.array([o[0] for o in offsets], jnp.int32)
    step_y = jnp.array([o[1] for o in offsets], jnp.int32)
    step_z = jnp.array([o[2] for o in offsets], jnp.int32)
    codes = jnp.array([9 * (o[0] + 1) + 3 * (o[1] + 1) + (o[2] + 1) for o in offsets], jnp.int32)
    block_total = PATCH_DEV * NBLK
    base = jax.random.fold_in(key, 1301)

    def single(device):
        device_key = jax.random.fold_in(base, device)
        key_fav, key_score, key_assign = jax.random.split(device_key, 3)
        favored = jax.random.randint(key_fav, (), 0, offset_total)
        pairs = jnp.arange(offset_total * CAP, dtype=jnp.int32)
        scores = jax.random.permutation(key_score, offset_total * CAP).astype(jnp.int32)
        scores = jnp.where(pairs // CAP == favored, scores - offset_total * CAP, scores)
        ranked = jnp.argsort(scores, stable=True).astype(jnp.int32)
        chosen = ranked[:block_total]
        picked = chosen[jax.random.permutation(key_assign, block_total).astype(jnp.int32)]
        offset_ids = picked // CAP
        slot_ids = (picked % CAP).astype(jnp.int32)
        coord_x = device // (PY * PZ)
        coord_y = device // PZ % PY
        coord_z = device % PZ
        owner_ids = ((coord_x + step_x[offset_ids]) % PX * PY * PZ + (coord_y + step_y[offset_ids]) % PY * PZ + (coord_z + step_z[offset_ids]) % PZ).astype(jnp.int32)
        return (owner_ids, slot_ids, codes[offset_ids])
    owner_all, slot_all, code_all = jax.vmap(single)(jnp.arange(NDEV, dtype=jnp.int32))
    target_all = jax.random.randint(jax.random.fold_in(key, 2417), (NDEV, block_total), 0, OWNB).astype(jnp.int32)
    index_all = (owner_all * 27 * CAP + code_all * CAP + slot_all).reshape(-1)
    target_table = jnp.full((NDEV * 27 * CAP,), -1, jnp.int32).at[index_all].set(target_all.reshape(-1))
    return (owner_all.reshape(NDEV * PATCH_DEV, NBLK), slot_all.reshape(NDEV * PATCH_DEV, NBLK), target_table.reshape(NDEV, 27, CAP))


def draw_block_owner(key, part):
    return routing(key)[0]


def draw_block_slot(key, part):
    return routing(key)[1]


def draw_recv_target(key, part):
    return routing(key)[2]


def block_levels(key, shape, shards, least, top_value):
    loudness, own = 1.0, jax.random.fold_in(key, 6)
    for axis_at, shards_of in shards:
        heights = jnp.exp(jax.random.uniform(jax.random.fold_in(own, axis_at), (shards_of,), jnp.float32, least / len(shards), top_value / len(shards)))
        loudness = loudness * jnp.repeat(heights, shape[axis_at] // shards_of).reshape([-1 if axis == axis_at else 1 for axis in range(len(shape))])
    return loudness


def noise(own_key, dims, width, most, cuts=(), held_as=jnp.bfloat16):
    loudness = block_levels(own_key, dims, cuts, -0.22, 0.18) if cuts else 1.0
    values = jax.random.normal(own_key, dims, jnp.float32) * width * loudness
    return jnp.minimum(jnp.maximum(values, -most), most).astype(held_as)


def setup_inputs(seed: int = 0) -> dict:
    seeds = jax.random.split(jax.random.key(seed), 6)
    star_residual = noise(seeds[0], (PATCHES, RHS, PDOF), 1.0, 6.0, ((0, 32),))
    patch_inverse = noise(seeds[1], (PATCHES, PDOF, PDOF), PDOF ** -0.5, 0.1875, ((0, 32),))
    block_owner = draw_block_owner(jax.random.fold_in(seeds[5], 71), 0)
    block_slot = draw_block_slot(jax.random.fold_in(seeds[5], 71), 0)
    recv_target = draw_recv_target(jax.random.fold_in(seeds[5], 71), 0)
    return dict(star_residual=star_residual, patch_inverse=patch_inverse, block_owner=block_owner, block_slot=block_slot, recv_target=recv_target)


def axis_code(far_index, near_index, extent):
    distance = (far_index - near_index) % extent
    return jnp.where(distance == 0, 1, jnp.where(distance == 1, 2, 0)).astype(jnp.int32)


def offset_code(owner_ids, sender_ids):
    owner_x = owner_ids // (PY * PZ)
    owner_y = (owner_ids // PZ) % PY
    owner_z = owner_ids % PZ
    sender_x = sender_ids // (PY * PZ)
    sender_y = (sender_ids // PZ) % PY
    sender_z = sender_ids % PZ
    return (9 * axis_code(owner_x, sender_x, PX) + 3 * axis_code(owner_y, sender_y, PY)
            + axis_code(owner_z, sender_z, PZ)).astype(jnp.int32)


def reference(star_residual, patch_inverse, block_owner, block_slot, recv_target):
    residual_wide = star_residual.astype(jnp.float32)
    inverse_wide = patch_inverse.astype(jnp.float32).reshape(PATCHES, NBLK, BW, PDOF)
    contribution = jnp.einsum('prj,pbwj->pbrw', residual_wide, inverse_wide, precision=lax.Precision.HIGHEST)
    blocks = contribution.reshape(PATCHES * NBLK, RHS, BW)
    sender_ids = (jnp.arange(PATCHES * NBLK, dtype=jnp.int32) // (PATCH_DEV * NBLK)).astype(jnp.int32)
    owner_ids = block_owner.reshape(-1).astype(jnp.int32)
    slot_ids = block_slot.reshape(-1).astype(jnp.int32)
    codes = offset_code(owner_ids, sender_ids)
    targets = recv_target[owner_ids, codes, slot_ids].astype(jnp.int32)
    keys = (owner_ids * OWNB + targets).astype(jnp.int32)
    owned_sum = jax.ops.segment_sum(blocks, keys, num_segments=NDEV * OWNB)
    combined = owned_sum[keys].reshape(PATCHES, NBLK, RHS, BW)
    return owned_sum, combined
```

```python
import functools

import jax
import jax.numpy as jnp
from jax import lax
from jax.experimental import pallas as pl
from jax.experimental.pallas import tpu as pltpu
from jax.sharding import PartitionSpec as P

OWNB = 8
CHUNKS = 4
VMEM_BYTES = 67043328
SPARE = 131072
MESH = pl.DeviceIdType.MESH


def offsets(extent):
    return [0, 1, -1][: min(extent, 3)]


def offset_index(far, near, extent):
    step = far - near
    distance = jnp.where(step < 0, step + extent, step)
    return jnp.where(distance <= 1, distance, 2)


def role_of(at, here):
    return jnp.where((at > 0) & (lax.rem(here, 2) == 1), 3 - at, at)


def partner(here, role, extent):
    step = 1 - 2 * (here % 2)
    return (here + (0, step, extent - step)[role]) % extent


def role_code(here, role):
    parity = here % 2
    return (1, 2 * parity, 2 - 2 * parity)[role]


def kernel(cfg, owner_hbm, slot_hbm, table_hbm, star_hbm, inv_hbm, owned_ref, comb_ref,
           owner_ref, slot_ref, table_ref, key_out, src_out, key_ref, src_ref,
           star, inv, made, sent, came, tgt_out, tgt, wide_out, wide,
           pd, px, wp, ry, rx, rw, own, g1, g2, w1, ans,
           index_sem, load_sem, t_send, t_recv, a_send, a_recv, b_send, b_recv, out_send, out_recv, *back):
    nx, ny, nz, chunks, capacity = cfg
    gx, gy, gz = lax.axis_index("gx"), lax.axis_index("gy"), lax.axis_index("gz")
    patch_count, block_count = owner_hbm.shape
    total = patch_count * block_count
    rows, lanes = came.shape[2], came.shape[3]
    steps = offsets(ny)
    ly = len(steps)

    def at(role_x, dy, role_z):
        return (partner(gx, role_x, nx), (gy + dy + ny) % ny, partner(gz, role_z, nz))

    near_x, corner, far_z = at(1, 0, 0), at(2, 0, 0), at(0, 0, 2)
    near_y = ((gx + nx // 2) % nx, gy, gz)

    groups = [[(rz, d, r) for rz in (0, 1) for d in range(ly)] for r in range(3)]
    groups.append([(2, d, r) for r in range(3) for d in range(ly)])
    bases = [2 * ly * r * capacity for r in range(4)]

    def route(part, sign):
        rz, d, r = part
        dy = sign * steps[d]
        return at(r, dy, 0) if rz == 2 else at(0, dy, rz)

    indices = [
        pltpu.make_async_copy(source, target, index_sem.at[i])
        for i, (source, target) in enumerate(
            ((owner_hbm, owner_ref), (slot_hbm, slot_ref), (table_hbm, table_ref)))]
    loads = [pltpu.make_async_copy(star_hbm, star, load_sem.at[patch_count])]
    for p in range(patch_count):
        loads.append(pltpu.make_async_copy(inv_hbm.at[p], inv.at[p], load_sem.at[p]))
    for load in indices + loads[:2]:
        load.start()

    barrier = pltpu.get_barrier_semaphore()
    greeted = [at(0, dy, rz) for dy in steps for rz in (0, 1) if dy or rz]
    greeted += [at(r, dy, 0) for dy in steps for r in (1, 2)] + [far_z, near_y]
    for device in greeted:
        pl.semaphore_signal(barrier, inc=1, device_id=device, device_id_type=MESH)

    for load in indices:
        load.wait()
    for load in loads[2:]:
        load.start()

    owner = owner_ref[...]
    owner_x = sum(((owner >= i * ny * nz).astype(jnp.int32) for i in range(1, nx)), jnp.zeros_like(owner))
    owner = owner - owner_x * (ny * nz)
    owner_y = sum(((owner >= i * nz).astype(jnp.int32) for i in range(1, ny)), jnp.zeros_like(owner))
    role_x = role_of(offset_index(owner_x, gx, nx), gx)
    at_y = offset_index(owner_y, gy, ny)
    role_z = role_of(offset_index(owner - owner_y * nz, gz, nz), gz)
    where = jnp.where(role_z == 2, 6 * ly + role_x * ly + at_y, (2 * role_x + role_z) * ly + at_y)
    key = where * capacity + slot_ref[...]
    key_out[0:patch_count, 0:block_count] = key
    tall = src_out.shape[0]
    number = lax.broadcasted_iota(jnp.int32, (tall, block_count), 0)
    block = lax.broadcasted_iota(jnp.int32, (tall, block_count), 1)
    found = jnp.zeros((tall, block_count), jnp.int32)
    for p in range(patch_count):
        hit = jnp.broadcast_to(key[p:p + 1, :], (tall, block_count)) == number
        found = jnp.maximum(found, jnp.where(hit, block + p * block_count, 0))
    src_out[...] = jnp.broadcast_to(
        jnp.max(found, axis=1, keepdims=True), src_out.shape)
    scalars = [
        pltpu.make_async_copy(key_out, key_ref, index_sem.at[0]),
        pltpu.make_async_copy(src_out, src_ref, index_sem.at[1])]
    for load in scalars:
        load.start()

    def entry(role_x, dy, role_z, s):
        code = 9 * role_code(gx, role_x) + 3 * (dy + 1) + role_code(gz, role_z)
        return jnp.full((1, lanes), table_ref[0, s, code], jnp.int32)

    for g, parts in enumerate(groups):
        for i, (rz, d, r) in enumerate(parts):
            for s in range(capacity):
                j = i * capacity + s
                if g == 3:
                    wide_out[j:j + 1, :] = entry(r, steps[d], rz, s)
                elif g:
                    tgt_out[g, j:j + 1, :] = entry(r, steps[d], rz, s)
                else:
                    tgt[g, j:j + 1, :] = entry(r, steps[d], rz, s)

    loads[0].wait()
    for p in range(patch_count):
        loads[1 + p].wait()
        block = lax.dot_general(
            star[p], inv[p], (((1,), (1,)), ((), ())), preferred_element_type=jnp.float32)
        for b in range(block_count):
            made[p * block_count + b] = block[:, b * lanes:(b + 1) * lanes]

    for load in scalars:
        load.wait()
    pl.semaphore_wait(barrier, len(greeted))

    def launch(source, target, send_sem, recv_sem, device):
        copy = pltpu.make_async_remote_copy(
            src_ref=source, dst_ref=target, send_sem=send_sem, recv_sem=recv_sem,
            device_id=device, device_id_type=MESH)
        copy.start()
        return copy

    t_copies = [
        launch(wide_out, wide, t_send.at[2], t_recv.at[2], far_z),
        launch(tgt_out.at[1], tgt.at[1], t_send.at[0], t_recv.at[0], near_x),
        launch(tgt_out.at[2], tgt.at[2], t_send.at[1], t_recv.at[1], corner),
    ]

    def piece(ref, c, slots):
        return ref[c].at[slots] if isinstance(ref, tuple) else ref.at[c, slots]

    def send_part(source, target, sends, recvs, g, i, c, sign):
        k = bases[g] + i * capacity
        launch(piece(source, c, pl.ds(k, capacity)), piece(target, c, pl.ds(k, capacity)),
               sends.at[g], recvs.at[g, c], route(groups[g][i], sign))

    def await_group(source, target, recvs, g, c):
        many = pl.ds(bases[g] + capacity, (len(groups[g]) - 1) * capacity)
        pltpu.make_async_copy(piece(source, c, many), piece(target, c, many), recvs.at[g, c]).wait()

    def pick(g, i):
        held = sent if i else came
        for s in range(capacity):
            k = bases[g] + i * capacity + s
            n = jnp.clip(src_ref[k, 0], 0, total - 1)
            for c in range(chunks):
                held[c, k] = made[n, c * rows:(c + 1) * rows, :]

    near = [(g, i) for g in (2, 1, 0) for i in range(ly, 2 * ly)]
    wide_parts = [(3, i) for i in reversed(range(1, 3 * ly))]
    beside = [(g, i) for g in (2, 1, 0) for i in range(1, ly)]

    def send_near(c):
        for g, i in near:
            send_part(sent, came, a_send, a_recv, g, i, c, 1)

    for g, i in near:
        pick(g, i)
        send_part(sent, came, a_send, a_recv, g, i, 0, 1)
    for g, i in wide_parts:
        pick(g, i)
        send_part(sent, came, a_send, a_recv, g, i, 0, 1)
    for g, i in beside:
        pick(g, i)
        send_part(sent, came, a_send, a_recv, g, i, 0, 1)
    for g in range(4):
        pick(g, 0)
    ahead = max(1, chunks // 2)
    for c in range(1, chunks):
        if c < ahead:
            send_near(c)
        for g, i in wide_parts + beside:
            send_part(sent, came, a_send, a_recv, g, i, c, 1)

    def where_of(g, j):
        row = wide[j:j + 1, :] if g == 3 else tgt[g, j:j + 1, :]
        return jnp.broadcast_to(row, (8, lanes))

    def reduce(g, c, added, out):
        await_group(sent, came, a_recv, g, c)
        for r in range(rows // 8):
            at_rows = pl.ds(r * 8, 8)
            sums = [None] * OWNB
            for t in range(OWNB):
                for ref in added:
                    value = ref[c, t, at_rows, :]
                    sums[t] = value if sums[t] is None else sums[t] + value
            for j in range(len(groups[g]) * capacity):
                value = came[c, bases[g] + j, at_rows, :]
                where = where_of(g, j)
                for t in range(OWNB):
                    term = jnp.where(where == t, value, 0.0)
                    sums[t] = term if sums[t] is None else sums[t] + term
            for t in range(OWNB):
                out[c, t, at_rows, :] = sums[t]

    def answer(g, c, held):
        for r in range(rows // 8):
            at_rows = pl.ds(r * 8, 8)
            values = [held[c, t, at_rows, :] for t in range(OWNB)]
            for j in range(len(groups[g]) * capacity):
                where = where_of(g, j)
                out = values[0]
                for t in range(1, OWNB):
                    out = jnp.where(where == t, values[t], out)
                into = ans.at[c] if j >= capacity else back[c]
                into[bases[g] + j, at_rows, :] = out
        for i in reversed(range(1, len(groups[g]))):
            send_part(ans, back, b_send, b_recv, g, i, c, -1)

    outs = ((pd, ry, near_y), (px, rx, near_x), (wp, rw, far_z),
            (own, g1, near_x), (g1, g2, near_y), (own, w1, far_z))

    def pass_on(kind, c):
        source, target, device = outs[kind]
        launch(source.at[c], target.at[c], out_send.at[kind], out_recv.at[kind, c], device)

    def await_out(kind, c):
        source, target, _ = outs[kind]
        pltpu.make_async_copy(source.at[c], target.at[c], out_recv.at[kind, c]).wait()

    def sum_proxied(c):
        if c == 0:
            t_copies[0].wait_recv()
        reduce(3, c, [], wp)
        pass_on(2, c)
        if c + ahead < chunks:
            send_near(c + ahead)

    def sum_corner(c):
        if c == 0:
            t_copies[2].wait_recv()
        reduce(2, c, [], pd)
        pass_on(0, c)

    def sum_near(c):
        if c == 0:
            t_copies[1].wait_recv()
        await_out(0, c)
        reduce(1, c, [ry], px)
        pass_on(1, c)

    def sum_own(c):
        await_out(1, c)
        await_out(2, c)
        reduce(0, c, [rx, rw], own)
        pass_on(5, c)
        pass_on(3, c)
        answer(0, c, own)
        for t in range(OWNB):
            owned_ref[t, pl.ds(c * rows, rows), :] = own[c, t]

    def back_near(c):
        await_out(3, c)
        pass_on(4, c)
        answer(1, c, g1)

    def back_proxied(c):
        await_out(5, c)
        answer(3, c, w1)

    def back_corner(c):
        await_out(4, c)
        answer(2, c, g2)

    def finish(c):
        for g in range(4):
            await_group(ans, back, b_recv, g, c)

        def place(p, carry):
            for b in range(block_count):
                comb_ref[p * block_count + b, pl.ds(c * rows, rows), :] = back[c][jnp.clip(key_ref[p, b], 0, came.shape[1] - 1)]
            return carry

        lax.fori_loop(0, patch_count, place, 0)

    plan = [
        (sum_corner, 9.5, 2.8), (sum_proxied, 9.8, 2.1), (sum_near, 13.2, 2.8), (sum_own, 17.0, 3.0),
        (back_near, 20.6, 3.0), (back_proxied, 25.5, 2.1), (back_corner, 24.2, 3.0), (finish, 37.0, 1.0),
    ]
    timed = [(start + every * 4.0 / chunks * c, i, c) for i, (_, start, every) in enumerate(plan) for c in range(chunks)]
    for _, i, c in sorted(timed):
        plan[i][0](c)

    for copy in t_copies:
        copy.wait_send()
    for g, parts in enumerate(groups):
        many = pl.ds(bases[g] + capacity, (len(parts) - 1) * capacity)
        for source, sends in ((sent, a_send), (ans, b_send)):
            pltpu.make_async_copy(source.at[:, many], came.at[:, many], sends.at[g]).wait()
    for kind, (source, target, _) in enumerate(outs):
        pltpu.make_async_copy(source, target, out_send.at[kind]).wait()


def store_kernel(owned_ref, comb_ref, owned_hbm, comb_hbm, sem):
    copies = [
        pltpu.make_async_copy(comb_ref, comb_hbm, sem.at[0]),
        pltpu.make_async_copy(owned_ref, owned_hbm, sem.at[1])]
    for copy in copies:
        copy.start()
    for copy in copies:
        copy.wait()


def on_device(star_residual, patch_inverse, block_owner, block_slot, recv_target):
    nx, ny, nz = lax.axis_size("gx"), lax.axis_size("gy"), lax.axis_size("gz")
    patch_count, rhs_count, patch_order = star_residual.shape
    block_count = block_owner.shape[1]
    width = patch_order // block_count
    capacity = recv_target.shape[2]
    total = patch_count * block_count
    ly = len(offsets(ny))
    slots = 9 * ly * capacity
    tall = -(-slots // 8) * 8
    chunks = CHUNKS
    rows = rhs_count // chunks
    hbm = pl.BlockSpec(memory_space=pltpu.HBM)
    vmem = pl.BlockSpec(memory_space=pltpu.VMEM)
    anywhere = pl.BlockSpec(memory_space=pl.ANY)
    f32, i32 = jnp.float32, jnp.int32
    slotted = pltpu.VMEM((chunks, slots, rows, width), f32)
    targeted = pltpu.VMEM((chunks, OWNB, rows, width), f32)
    table = pltpu.VMEM((3, 2 * ly * capacity, width), i32)
    wide = pltpu.VMEM((3 * ly * capacity, width), i32)
    dma = pltpu.SemaphoreType.DMA
    limit = VMEM_BYTES - SPARE - (OWNB + total) * rhs_count * width * 4
    owned, comb = pl.pallas_call(
        functools.partial(kernel, (nx, ny, nz, chunks, capacity)),
        out_shape=(
            pltpu.VMEM((OWNB, rhs_count, width), f32),
            pltpu.VMEM((total, rhs_count, width), f32),
        ),
        in_specs=[hbm] * 5,
        out_specs=(vmem, vmem),
        scratch_shapes=[
            pltpu.VMEM(block_owner.shape, i32),
            pltpu.VMEM(block_slot.shape, i32),
            pltpu.SMEM((1, capacity, recv_target.shape[1]), i32),
            pltpu.VMEM((8, 128), i32),
            pltpu.VMEM((tall, 128), i32),
            pltpu.SMEM((8, 128), i32),
            pltpu.SMEM((tall, 128), i32),
            pltpu.VMEM(star_residual.shape, star_residual.dtype),
            pltpu.VMEM(patch_inverse.shape, patch_inverse.dtype),
            pltpu.VMEM((total, rhs_count, width), f32),
            slotted, slotted,
            table, table, wide, wide,
            targeted, targeted, targeted, targeted, targeted, targeted, targeted, targeted, targeted, targeted,
            slotted,
            dma((3,)), dma((patch_count + 1,)), dma((3,)), dma((3,)),
            dma((4,)), dma((4, chunks)), dma((4,)), dma((4, chunks)),
            dma((6,)), dma((6, chunks)),
        ] + [pltpu.VMEM((slots, rows, width), f32)] * chunks,
        compiler_params=pltpu.CompilerParams(
            collective_id=0, has_side_effects=True, vmem_limit_bytes=limit),
    )(block_owner, block_slot, recv_target.transpose(0, 2, 1), star_residual, patch_inverse)
    owned, comb = pl.pallas_call(
        store_kernel,
        out_shape=(
            jax.ShapeDtypeStruct((OWNB, rhs_count, width), f32),
            jax.ShapeDtypeStruct((total, rhs_count, width), f32),
        ),
        in_specs=[anywhere, anywhere],
        out_specs=(anywhere, anywhere),
        scratch_shapes=[dma((2,))],
        compiler_params=pltpu.CompilerParams(vmem_limit_bytes=1024 * 1024),
    )(owned, comb)
    return owned, comb.reshape(patch_count, block_count, rhs_count, width)


def solution(mesh):
    placed = (
        P(("gx", "gy", "gz"), None, None),
        P(("gx", "gy", "gz"), None, None),
        P(("gx", "gy", "gz"), None),
        P(("gx", "gy", "gz"), None),
        P(("gx", "gy", "gz"), None, None),
    )
    return jax.shard_map(
        on_device,
        mesh=mesh,
        in_specs=placed,
        out_specs=(P(("gx", "gy", "gz"), None, None), P(("gx", "gy", "gz"), None, None, None)),
        check_vma=False,
    )
```

```python
import functools

import jax
import jax.numpy as jnp
from jax import lax
from jax.experimental import pallas as pl
from jax.experimental.pallas import tpu as pltpu
from jax.sharding import PartitionSpec as P

OWNB = 8
CHUNKS = 4
RAW_OUT = 2
RAW_BACK = 1
VMEM_BYTES = 67043328
SPARE = 131072
MESH = pl.DeviceIdType.MESH


def offsets(extent):
    return [0, 1, -1][: min(extent, 3)]


def offset_index(far, near, extent):
    step = far - near
    distance = jnp.where(step < 0, step + extent, step)
    return jnp.where(distance <= 1, distance, 2)


def role_of(at, here):
    return jnp.where((at > 0) & (lax.rem(here, 2) == 1), 3 - at, at)


def partner(here, role, extent):
    step = 1 - 2 * (here % 2)
    return (here + (0, step, extent - step)[role]) % extent


def role_code(here, role):
    parity = here % 2
    return (1, 2 * parity, 2 - 2 * parity)[role]


def kernel(cfg, owner_hbm, slot_hbm, table_hbm, star_hbm, inv_hbm, owned_ref, comb_ref,
           owner_ref, slot_ref, table_ref, key_out, src_out, key_ref, src_ref,
           star, inv, made, sent, came, tgt_out, tgt, wide_out, wide,
           pd, px, wp, ry, rx, rw, own, g1, g2, w1, ans,
           index_sem, load_sem, t_send, t_recv, a_send, a_recv, b_send, b_recv, out_send, out_recv,
           f_send, f_recv, e_send, e_recv, *back):
    nx, ny, nz, chunks, capacity = cfg
    gx, gy, gz = lax.axis_index("gx"), lax.axis_index("gy"), lax.axis_index("gz")
    patch_count, block_count = owner_hbm.shape
    total = patch_count * block_count
    rows, lanes = came.shape[2], came.shape[3]
    steps = offsets(ny)
    ly = len(steps)

    def at(role_x, dy, role_z):
        return (partner(gx, role_x, nx), (gy + dy + ny) % ny, partner(gz, role_z, nz))

    near_x, corner, far_z = at(1, 0, 0), at(2, 0, 0), at(0, 0, 2)
    near_y = ((gx + nx // 2) % nx, gy, gz)

    groups = [[(rz, d, r) for rz in (0, 1) for d in range(ly)] for r in range(3)]
    groups.append([(2, d, r) for r in range(3) for d in range(ly)])
    bases = [2 * ly * r * capacity for r in range(4)]
    raw_out, raw_back = min(RAW_OUT, chunks), chunks - min(RAW_BACK, chunks)
    inner = (gz > 0) & (gz < nz - 1)
    outer = jnp.logical_not(inner)

    def far_slots(r):
        return pl.ds(bases[3] + r * ly * capacity, ly * capacity)

    every_far = pl.ds(bases[3], 3 * ly * capacity)

    def route(part, sign):
        rz, d, r = part
        dy = sign * steps[d]
        return at(r, dy, 0) if rz == 2 else at(0, dy, rz)

    indices = [
        pltpu.make_async_copy(source, target, index_sem.at[i])
        for i, (source, target) in enumerate(
            ((owner_hbm, owner_ref), (slot_hbm, slot_ref), (table_hbm, table_ref)))]
    half = block_count // 2 * lanes
    loads = [pltpu.make_async_copy(star_hbm, star, load_sem.at[patch_count])]
    spans = [(0, 0, half), (0, half, block_count * lanes)]
    spans += [(p, 0, block_count * lanes) for p in range(1, patch_count)]
    for i, (p, low, high) in enumerate(spans):
        span = pl.ds(low, high - low)
        sem = load_sem.at[p if i else patch_count + 1]
        loads.append(pltpu.make_async_copy(inv_hbm.at[p, span], inv.at[p, span], sem))
    for load in indices + loads[:3]:
        load.start()

    barrier = pltpu.get_barrier_semaphore()
    greeted = [at(0, dy, rz) for dy in steps for rz in (0, 1, 2) if dy or rz]
    greeted += [at(r, dy, 0) for dy in steps for r in (1, 2)] + [near_y]
    for device in greeted:
        pl.semaphore_signal(barrier, inc=1, device_id=device, device_id_type=MESH)

    for load in indices:
        load.wait()
    for load in loads[3:]:
        load.start()

    def multiply(i):
        p, low, high = spans[i]
        loads[1 + i].wait()
        block = lax.dot_general(
            star[p], inv[p, low:high, :], (((1,), (1,)), ((), ())), preferred_element_type=jnp.float32)
        for b in range((high - low) // lanes):
            made[p * block_count + low // lanes + b] = block[:, b * lanes:(b + 1) * lanes]

    loads[0].wait()
    multiply(0)
    multiply(1)

    owner = owner_ref[...]
    owner_x = sum(((owner >= i * ny * nz).astype(jnp.int32) for i in range(1, nx)), jnp.zeros_like(owner))
    owner = owner - owner_x * (ny * nz)
    owner_y = sum(((owner >= i * nz).astype(jnp.int32) for i in range(1, ny)), jnp.zeros_like(owner))
    role_x = role_of(offset_index(owner_x, gx, nx), gx)
    at_y = offset_index(owner_y, gy, ny)
    role_z = role_of(offset_index(owner - owner_y * nz, gz, nz), gz)
    where = jnp.where(role_z == 2, 6 * ly + role_x * ly + at_y, (2 * role_x + role_z) * ly + at_y)
    key = where * capacity + slot_ref[...]
    key_out[0:patch_count, 0:block_count] = key
    tall = src_out.shape[0]
    number = lax.broadcasted_iota(jnp.int32, (tall, block_count), 0)
    block = lax.broadcasted_iota(jnp.int32, (tall, block_count), 1)
    found = jnp.zeros((tall, block_count), jnp.int32)
    for p in range(patch_count):
        hit = jnp.broadcast_to(key[p:p + 1, :], (tall, block_count)) == number
        found = jnp.maximum(found, jnp.where(hit, block + p * block_count, 0))
    src_out[...] = jnp.broadcast_to(
        jnp.max(found, axis=1, keepdims=True), src_out.shape)
    scalars = [
        pltpu.make_async_copy(key_out, key_ref, index_sem.at[0]),
        pltpu.make_async_copy(src_out, src_ref, index_sem.at[1])]
    for load in scalars:
        load.start()

    def entry(role_x, dy, role_z, s):
        code = 9 * role_code(gx, role_x) + 3 * (dy + 1) + role_code(gz, role_z)
        return jnp.full((1, lanes), table_ref[0, s, code], jnp.int32)

    for r in range(3):
        for rz in range(3):
            for d, dy in enumerate(steps):
                for s in range(capacity):
                    row = entry(r, dy, rz, s)
                    j = (rz * ly + d) * capacity + s
                    held = tgt_out if r else tgt
                    held[r, j:j + 1, :] = row
                    if rz == 2:
                        j = (r * ly + d) * capacity + s
                        wide_out[j:j + 1, :] = row

    for i in range(2, len(spans) - 1):
        multiply(i)

    pl.semaphore_wait(barrier, len(greeted))

    def launch(source, target, send_sem, recv_sem, device):
        copy = pltpu.make_async_remote_copy(
            src_ref=source, dst_ref=target, send_sem=send_sem, recv_sem=recv_sem,
            device_id=device, device_id_type=MESH)
        copy.start()
        return copy

    t_copies = [
        launch(wide_out, wide, t_send.at[2], t_recv.at[2], far_z),
        launch(tgt_out.at[1], tgt.at[1], t_send.at[0], t_recv.at[0], near_x),
        launch(tgt_out.at[2], tgt.at[2], t_send.at[1], t_recv.at[1], corner),
    ]

    multiply(len(spans) - 1)
    for load in scalars:
        load.wait()

    def piece(ref, c, slots):
        return ref[c].at[slots] if isinstance(ref, tuple) else ref.at[c, slots]

    def send_part(source, target, sends, recvs, g, i, c, sign):
        k = bases[g] + i * capacity
        launch(piece(source, c, pl.ds(k, capacity)), piece(target, c, pl.ds(k, capacity)),
               sends.at[g], recvs.at[g, c], route(groups[g][i], sign))

    def await_group(source, target, recvs, g, c):
        many = pl.ds(bases[g] + capacity, (len(groups[g]) - 1) * capacity)
        pltpu.make_async_copy(piece(source, c, many), piece(target, c, many), recvs.at[g, c]).wait()

    def pick(g, i):
        for s in range(capacity):
            k = bases[g] + i * capacity + s
            n = jnp.clip(src_ref[k, 0], 0, total - 1)
            for c in range(chunks):
                value = made[n, c * rows:(c + 1) * rows, :]
                if i or (g == 3 and c < raw_out):
                    sent[c, k] = value
                if not i:
                    if g == 3 and c < raw_out:
                        @pl.when(outer)
                        def _():
                            came[c, k] = value
                    else:
                        came[c, k] = value

    def send_far(c):
        @pl.when(inner)
        def _():
            for r in (2, 1, 0):
                for d in reversed(range(ly)):
                    k = pl.ds(bases[3] + (r * ly + d) * capacity, capacity)
                    launch(sent.at[c, k], came.at[c, k], f_send, f_recv.at[r, c], at(0, steps[d], 2))

        @pl.when(outer)
        def _():
            for g, i in wide_parts:
                k = pl.ds(bases[g] + i * capacity, capacity)
                launch(sent.at[c, k], came.at[c, k], f_send, a_recv.at[g, c], route(groups[g][i], 1))

    near = [(g, i) for g in (2, 1, 0) for i in range(ly, 2 * ly)]
    wide_parts = [(3, i) for i in reversed(range(1, 3 * ly))]
    beside = [(g, i) for g in (2, 1, 0) for i in range(1, ly)]

    def send_near(c):
        for g, i in near:
            send_part(sent, came, a_send, a_recv, g, i, c, 1)

    for g, i in near:
        pick(g, i)
        send_part(sent, came, a_send, a_recv, g, i, 0, 1)
    for g, i in wide_parts + [(3, 0)]:
        pick(g, i)
    if raw_out:
        send_far(0)
    else:
        for g, i in wide_parts:
            send_part(sent, came, a_send, a_recv, g, i, 0, 1)
    for g, i in beside:
        pick(g, i)
        send_part(sent, came, a_send, a_recv, g, i, 0, 1)
    for g in range(3):
        pick(g, 0)
    ahead = max(1, chunks // 2)
    for c in range(1, chunks):
        if c < ahead:
            send_near(c)
        if c < raw_out:
            send_far(c)
        for g, i in ([] if c < raw_out else wide_parts) + beside:
            send_part(sent, came, a_send, a_recv, g, i, c, 1)

    def where_of(g, j):
        row = wide[j:j + 1, :] if g == 3 else tgt[g, j:j + 1, :]
        return jnp.broadcast_to(row, (8, lanes))

    def reduce(g, c, added, out):
        await_group(sent, came, a_recv, g, c)
        for r in range(rows // 8):
            at_rows = pl.ds(r * 8, 8)
            sums = [None] * OWNB
            for t in range(OWNB):
                for ref in added:
                    value = ref[c, t, at_rows, :]
                    sums[t] = value if sums[t] is None else sums[t] + value
            for j in range(len(groups[g]) * capacity):
                value = came[c, bases[g] + j, at_rows, :]
                where = where_of(g, j)
                for t in range(OWNB):
                    term = jnp.where(where == t, value, 0.0)
                    sums[t] = term if sums[t] is None else sums[t] + term
            for t in range(OWNB):
                out[c, t, at_rows, :] = sums[t]

    def add_far(g, c, out):
        pltpu.make_async_copy(sent.at[c, far_slots(g)], came.at[c, far_slots(g)], f_recv.at[g, c]).wait()
        for r in range(rows // 8):
            at_rows = pl.ds(r * 8, 8)
            sums = [out[c, t, at_rows, :] for t in range(OWNB)]
            for j in range(ly * capacity):
                value = came[c, bases[3] + g * ly * capacity + j, at_rows, :]
                where = where_of(g, 2 * ly * capacity + j)
                for t in range(OWNB):
                    sums[t] = sums[t] + jnp.where(where == t, value, 0.0)
            for t in range(OWNB):
                out[c, t, at_rows, :] = sums[t]

    def sum_role(g, c, added, out):
        reduce(g, c, added, out)
        if c < raw_out:
            @pl.when(inner)
            def _():
                add_far(g, c, out)

    def answer_far(g, c, held):
        for r in range(rows // 8):
            at_rows = pl.ds(r * 8, 8)
            values = [held[c, t, at_rows, :] for t in range(OWNB)]
            for j in range(ly * capacity):
                where = where_of(g, 2 * ly * capacity + j)
                out = values[0]
                for t in range(1, OWNB):
                    out = jnp.where(where == t, values[t], out)
                ans[c, bases[3] + g * ly * capacity + j, at_rows, :] = out
        for d in reversed(range(ly)):
            k = pl.ds(bases[3] + (g * ly + d) * capacity, capacity)
            launch(ans.at[c, k], back[c].at[k], e_send, e_recv.at[c], at(0, -steps[d], 2))

    def answer(g, c, held):
        if g < 3 and c >= raw_back:
            answer_part(g, c, held)

            @pl.when(inner)
            def _():
                answer_far(g, c, held)
        elif g == 3 and c >= raw_back:
            @pl.when(outer)
            def _():
                answer_part(g, c, held)
        else:
            answer_part(g, c, held)

    def answer_part(g, c, held):
        for r in range(rows // 8):
            at_rows = pl.ds(r * 8, 8)
            values = [held[c, t, at_rows, :] for t in range(OWNB)]
            for j in range(len(groups[g]) * capacity):
                where = where_of(g, j)
                out = values[0]
                for t in range(1, OWNB):
                    out = jnp.where(where == t, values[t], out)
                into = ans.at[c] if j >= capacity else back[c]
                into[bases[g] + j, at_rows, :] = out
        for i in reversed(range(1, len(groups[g]))):
            send_part(ans, back, b_send, b_recv, g, i, c, -1)

    outs = ((pd, ry, near_y), (px, rx, near_x), (wp, rw, far_z),
            (own, g1, near_x), (g1, g2, near_y), (own, w1, far_z))

    def pass_on(kind, c):
        source, target, device = outs[kind]
        launch(source.at[c], target.at[c], out_send.at[kind], out_recv.at[kind, c], device)

    def await_out(kind, c):
        source, target, _ = outs[kind]
        pltpu.make_async_copy(source.at[c], target.at[c], out_recv.at[kind, c]).wait()

    def sum_proxied(c):
        if c == 0:
            t_copies[0].wait_recv()

        def proxy():
            reduce(3, c, [], wp)
            pass_on(2, c)

        if c < raw_out:
            pl.when(outer)(proxy)
        else:
            proxy()
        if c + ahead < chunks:
            send_near(c + ahead)

    def sum_corner(c):
        if c == 0:
            t_copies[2].wait_recv()
        sum_role(2, c, [], pd)
        pass_on(0, c)

    def sum_near(c):
        if c == 0:
            t_copies[1].wait_recv()
        await_out(0, c)
        sum_role(1, c, [ry], px)
        pass_on(1, c)

    def sum_own(c):
        await_out(1, c)
        if c < raw_out:
            sum_role(0, c, [rx], own)

            @pl.when(outer)
            def _():
                await_out(2, c)
                own[c] = own[c] + rw[c]
        else:
            await_out(2, c)
            reduce(0, c, [rx, rw], own)
        if c >= raw_back:
            pl.when(outer)(lambda: pass_on(5, c))
        else:
            pass_on(5, c)
        pass_on(3, c)
        answer(0, c, own)
        for t in range(OWNB):
            owned_ref[t, pl.ds(c * rows, rows), :] = own[c, t]

    def back_near(c):
        await_out(3, c)
        pass_on(4, c)
        answer(1, c, g1)

    def back_proxied(c):
        if c >= raw_back:
            @pl.when(outer)
            def _():
                await_out(5, c)
                answer_part(3, c, w1)
        else:
            await_out(5, c)
            answer_part(3, c, w1)

    def back_corner(c):
        await_out(4, c)
        answer(2, c, g2)

    def finish(c):
        for g in range(3):
            await_group(ans, back, b_recv, g, c)
        if c >= raw_back:
            pl.when(outer)(lambda: await_group(ans, back, b_recv, 3, c))

            @pl.when(inner)
            def _():
                pltpu.make_async_copy(ans.at[c, every_far], back[c].at[every_far], e_recv.at[c]).wait()
        else:
            await_group(ans, back, b_recv, 3, c)

        def place(p, carry):
            for b in range(block_count):
                comb_ref[p * block_count + b, pl.ds(c * rows, rows), :] = back[c][jnp.clip(key_ref[p, b], 0, came.shape[1] - 1)]
            return carry

        lax.fori_loop(0, patch_count, place, 0)

    def drain(ref, low, high, slots, sem):
        if high > low:
            view = ref.at[pl.ds(low, high - low)] if slots is None else ref.at[pl.ds(low, high - low), slots]
            pltpu.make_async_copy(view, view, sem).wait()

    def drain_sums():
        for copy in t_copies:
            copy.wait_send()
        for g, parts in enumerate(groups):
            many = pl.ds(bases[g] + capacity, (len(parts) - 1) * capacity)
            drain(sent, raw_out if g == 3 else 0, chunks, many, a_send.at[g])
        pl.when(inner)(lambda: drain(sent, 0, raw_out, every_far, f_send))
        pl.when(outer)(lambda: drain(sent, 0, raw_out, many, f_send))
        for kind, (source, _, _) in enumerate(outs):
            if kind in (2, 5):
                low, high = (raw_out, chunks) if kind == 2 else (0, raw_back)
                pl.when(inner)(lambda: drain(source, low, high, None, out_send.at[kind]))
                pl.when(outer)(lambda: drain(source, 0, chunks, None, out_send.at[kind]))
            else:
                drain(source, 0, chunks, None, out_send.at[kind])

    plan = [
        (sum_corner, 9.5, 2.8), (sum_proxied, 9.8, 2.1), (sum_near, 13.2, 2.8), (sum_own, 17.0, 3.0),
        (back_near, 20.6, 3.0), (back_proxied, 30.5, 2.1), (back_corner, 24.2, 3.0), (finish, 37.0, 1.0),
    ]
    timed = [(start + every * 4.0 / chunks * c, i, c) for i, (_, start, every) in enumerate(plan) for c in range(chunks)]
    for _, i, c in sorted(timed):
        if (i, c) == (len(plan) - 1, chunks - 1):
            drain_sums()
        plan[i][0](c)

    def drain(ref, low, high, slots, sem):
        if high > low:
            view = ref.at[pl.ds(low, high - low)] if slots is None else ref.at[pl.ds(low, high - low), slots]
            pltpu.make_async_copy(view, view, sem).wait()

    for g, parts in enumerate(groups):
        many = pl.ds(bases[g] + capacity, (len(parts) - 1) * capacity)
        if g < 3:
            drain(ans, 0, chunks, many, b_send.at[g])
        else:
            @pl.when(inner)
            def _():
                drain(ans, 0, raw_back, many, b_send.at[3])
                drain(ans, raw_back, chunks, every_far, e_send)

            @pl.when(outer)
            def _():
                drain(ans, 0, chunks, many, b_send.at[3])


def store_kernel(owned_ref, comb_ref, owned_hbm, comb_hbm, sem):
    copies = [
        pltpu.make_async_copy(comb_ref, comb_hbm, sem.at[0]),
        pltpu.make_async_copy(owned_ref, owned_hbm, sem.at[1])]
    for copy in copies:
        copy.start()
    for copy in copies:
        copy.wait()


def on_device(star_residual, patch_inverse, block_owner, block_slot, recv_target):
    nx, ny, nz = lax.axis_size("gx"), lax.axis_size("gy"), lax.axis_size("gz")
    patch_count, rhs_count, patch_order = star_residual.shape
    block_count = block_owner.shape[1]
    width = patch_order // block_count
    capacity = recv_target.shape[2]
    total = patch_count * block_count
    ly = len(offsets(ny))
    slots = 9 * ly * capacity
    tall = -(-slots // 8) * 8
    chunks = CHUNKS
    rows = rhs_count // chunks
    hbm = pl.BlockSpec(memory_space=pltpu.HBM)
    vmem = pl.BlockSpec(memory_space=pltpu.VMEM)
    anywhere = pl.BlockSpec(memory_space=pl.ANY)
    f32, i32 = jnp.float32, jnp.int32
    slotted = pltpu.VMEM((chunks, slots, rows, width), f32)
    targeted = pltpu.VMEM((chunks, OWNB, rows, width), f32)
    table = pltpu.VMEM((3, 3 * ly * capacity, width), i32)
    wide = pltpu.VMEM((3 * ly * capacity, width), i32)
    dma = pltpu.SemaphoreType.DMA
    limit = VMEM_BYTES - SPARE - (OWNB + total) * rhs_count * width * 4
    owned, comb = pl.pallas_call(
        functools.partial(kernel, (nx, ny, nz, chunks, capacity)),
        out_shape=(
            pltpu.VMEM((OWNB, rhs_count, width), f32),
            pltpu.VMEM((total, rhs_count, width), f32),
        ),
        in_specs=[hbm] * 5,
        out_specs=(vmem, vmem),
        scratch_shapes=[
            pltpu.VMEM(block_owner.shape, i32),
            pltpu.VMEM(block_slot.shape, i32),
            pltpu.SMEM((1, capacity, recv_target.shape[1]), i32),
            pltpu.VMEM((8, 128), i32),
            pltpu.VMEM((tall, 128), i32),
            pltpu.SMEM((8, 128), i32),
            pltpu.SMEM((tall, 128), i32),
            pltpu.VMEM(star_residual.shape, star_residual.dtype),
            pltpu.VMEM(patch_inverse.shape, patch_inverse.dtype),
            pltpu.VMEM((total, rhs_count, width), f32),
            slotted, slotted,
            table, table, wide, wide,
            targeted, targeted, targeted, targeted, targeted, targeted, targeted, targeted, targeted, targeted,
            slotted,
            dma((3,)), dma((patch_count + 2,)), dma((3,)), dma((3,)),
            dma((4,)), dma((4, chunks)), dma((4,)), dma((4, chunks)),
            dma((6,)), dma((6, chunks)),
            dma, dma((3, chunks)), dma, dma((chunks,)),
        ] + [pltpu.VMEM((slots, rows, width), f32)] * chunks,
        compiler_params=pltpu.CompilerParams(
            collective_id=0, has_side_effects=True, vmem_limit_bytes=limit),
    )(block_owner, block_slot, recv_target.transpose(0, 2, 1), star_residual, patch_inverse)
    owned, comb = pl.pallas_call(
        store_kernel,
        out_shape=(
            jax.ShapeDtypeStruct((OWNB, rhs_count, width), f32),
            jax.ShapeDtypeStruct((total, rhs_count, width), f32),
        ),
        in_specs=[anywhere, anywhere],
        out_specs=(anywhere, anywhere),
        scratch_shapes=[dma((2,))],
        compiler_params=pltpu.CompilerParams(vmem_limit_bytes=1024 * 1024),
    )(owned, comb)
    return owned, comb.reshape(patch_count, block_count, rhs_count, width)


def solution(mesh):
    placed = (
        P(("gx", "gy", "gz"), None, None),
        P(("gx", "gy", "gz"), None, None),
        P(("gx", "gy", "gz"), None),
        P(("gx", "gy", "gz"), None),
        P(("gx", "gy", "gz"), None, None),
    )
    return jax.shard_map(
        on_device,
        mesh=mesh,
        in_specs=placed,
        out_specs=(P(("gx", "gy", "gz"), None, None), P(("gx", "gy", "gz"), None, None, None)),
        check_vma=False,
    )
```

```python
import functools

import jax
import jax.numpy as jnp
from jax import lax
from jax.experimental import pallas as pl
from jax.experimental.pallas import tpu as pltpu
from jax.sharding import PartitionSpec as P

OWNB = 8
CHUNKS = 4
EARLY_N = 3.5
EARLY_O = 2.5
EARLY_C = 3.0
RAW_OUT = 2
RAW_BACK = 2
STRAIGHT_OUT = 1
STRAIGHT_BACK = 1
VMEM_BYTES = 67043328
SPARE = 131072
MESH = pl.DeviceIdType.MESH


def offsets(extent):
    return [0, 1, -1][: min(extent, 3)]


def offset_index(far, near, extent):
    step = far - near
    distance = jnp.where(step < 0, step + extent, step)
    return jnp.where(distance <= 1, distance, 2)


def role_of(at, here):
    return jnp.where((at > 0) & (lax.rem(here, 2) == 1), 3 - at, at)


def partner(here, role, extent):
    step = 1 - 2 * (here % 2)
    return (here + (0, step, extent - step)[role]) % extent


def role_code(here, role):
    parity = here % 2
    return (1, 2 * parity, 2 - 2 * parity)[role]


def kernel(cfg, owner_hbm, slot_hbm, table_hbm, star_hbm, inv_hbm, owned_ref, comb_ref,
           owner_ref, slot_ref, table_ref, key_out, src_out, key_ref, src_ref,
           star, inv, made, sent, came, tgt_out, tgt, wide_out, wide,
           pd, px, wp, ry, rx, rw, own, g1, g2, w1, ans,
           index_sem, load_sem, t_send, t_recv, a_send, a_recv, b_send, b_recv, out_send, out_recv,
           f_send, f_recv, e_send, e_recv, *back):
    nx, ny, nz, chunks, capacity = cfg
    gx, gy, gz = lax.axis_index("gx"), lax.axis_index("gy"), lax.axis_index("gz")
    patch_count, block_count = owner_hbm.shape
    total = patch_count * block_count
    rows, lanes = came.shape[2], came.shape[3]
    steps = offsets(ny)
    ly = len(steps)

    def at(role_x, dy, role_z):
        return (partner(gx, role_x, nx), (gy + dy + ny) % ny, partner(gz, role_z, nz))

    near_x, corner, far_z = at(1, 0, 0), at(2, 0, 0), at(0, 0, 2)
    near_y = ((gx + nx // 2) % nx, gy, gz)

    groups = [[(rz, d, r) for rz in (0, 1) for d in range(ly)] for r in range(3)]
    groups.append([(2, d, r) for r in range(3) for d in range(ly)])
    bases = [2 * ly * r * capacity for r in range(4)]
    raw_out, raw_back = min(RAW_OUT, chunks), chunks - min(RAW_BACK, chunks)
    inner = (gz > 0) & (gz < nz - 1)
    outer = jnp.logical_not(inner)

    def far_slots(r):
        return pl.ds(bases[3] + r * ly * capacity, ly * capacity)

    every_far = pl.ds(bases[3], 3 * ly * capacity)

    def route(part, sign):
        rz, d, r = part
        dy = sign * steps[d]
        return at(r, dy, 0) if rz == 2 else at(0, dy, rz)

    indices = [
        pltpu.make_async_copy(source, target, index_sem.at[i])
        for i, (source, target) in enumerate(
            ((owner_hbm, owner_ref), (slot_hbm, slot_ref), (table_hbm, table_ref)))]
    half = block_count // 2 * lanes
    loads = [pltpu.make_async_copy(star_hbm, star, load_sem.at[patch_count])]
    spans = [(0, 0, half), (0, half, block_count * lanes)]
    spans += [(p, 0, block_count * lanes) for p in range(1, patch_count)]
    for i, (p, low, high) in enumerate(spans):
        span = pl.ds(low, high - low)
        sem = load_sem.at[p if i else patch_count + 1]
        loads.append(pltpu.make_async_copy(inv_hbm.at[p, span], inv.at[p, span], sem))
    for load in indices + loads[:3]:
        load.start()

    barrier = pltpu.get_barrier_semaphore()
    greeted = [at(0, dy, rz) for dy in steps for rz in (0, 1, 2) if dy or rz]
    greeted += [at(r, dy, 0) for dy in steps for r in (1, 2)] + [near_y]
    for device in greeted:
        pl.semaphore_signal(barrier, inc=1, device_id=device, device_id_type=MESH)

    for load in indices:
        load.wait()
    for load in loads[3:]:
        load.start()

    def multiply(i):
        p, low, high = spans[i]
        loads[1 + i].wait()
        block = lax.dot_general(
            star[p], inv[p, low:high, :], (((1,), (1,)), ((), ())), preferred_element_type=jnp.float32)
        for b in range((high - low) // lanes):
            made[p * block_count + low // lanes + b] = block[:, b * lanes:(b + 1) * lanes]

    loads[0].wait()
    multiply(0)
    multiply(1)

    owner = owner_ref[...]
    owner_x = sum(((owner >= i * ny * nz).astype(jnp.int32) for i in range(1, nx)), jnp.zeros_like(owner))
    owner = owner - owner_x * (ny * nz)
    owner_y = sum(((owner >= i * nz).astype(jnp.int32) for i in range(1, ny)), jnp.zeros_like(owner))
    role_x = role_of(offset_index(owner_x, gx, nx), gx)
    at_y = offset_index(owner_y, gy, ny)
    role_z = role_of(offset_index(owner - owner_y * nz, gz, nz), gz)
    where = jnp.where(role_z == 2, 6 * ly + role_x * ly + at_y, (2 * role_x + role_z) * ly + at_y)
    key = where * capacity + slot_ref[...]
    key_out[0:patch_count, 0:block_count] = key
    tall = src_out.shape[0]
    number = lax.broadcasted_iota(jnp.int32, (tall, block_count), 0)
    block = lax.broadcasted_iota(jnp.int32, (tall, block_count), 1)
    found = jnp.zeros((tall, block_count), jnp.int32)
    for p in range(patch_count):
        hit = jnp.broadcast_to(key[p:p + 1, :], (tall, block_count)) == number
        found = jnp.maximum(found, jnp.where(hit, block + p * block_count, 0))
    src_out[...] = jnp.broadcast_to(
        jnp.max(found, axis=1, keepdims=True), src_out.shape)
    scalars = [
        pltpu.make_async_copy(key_out, key_ref, index_sem.at[0]),
        pltpu.make_async_copy(src_out, src_ref, index_sem.at[1])]
    for load in scalars:
        load.start()

    def entry(role_x, dy, role_z, s):
        code = 9 * role_code(gx, role_x) + 3 * (dy + 1) + role_code(gz, role_z)
        return jnp.full((1, lanes), table_ref[0, s, code], jnp.int32)

    for r in range(3):
        for rz in range(3):
            for d, dy in enumerate(steps):
                for s in range(capacity):
                    row = entry(r, dy, rz, s)
                    j = (rz * ly + d) * capacity + s
                    held = tgt_out if r else tgt
                    held[r, j:j + 1, :] = row
                    if rz == 2:
                        j = (r * ly + d) * capacity + s
                        wide_out[j:j + 1, :] = row

    for i in range(2, len(spans) - 1):
        multiply(i)

    pl.semaphore_wait(barrier, len(greeted))

    def launch(source, target, send_sem, recv_sem, device):
        copy = pltpu.make_async_remote_copy(
            src_ref=source, dst_ref=target, send_sem=send_sem, recv_sem=recv_sem,
            device_id=device, device_id_type=MESH)
        copy.start()
        return copy

    t_copies = [
        launch(wide_out, wide, t_send.at[2], t_recv.at[2], far_z),
        launch(tgt_out.at[1], tgt.at[1], t_send.at[0], t_recv.at[0], near_x),
        launch(tgt_out.at[2], tgt.at[2], t_send.at[1], t_recv.at[1], corner),
    ]

    multiply(len(spans) - 1)
    for load in scalars:
        load.wait()

    def piece(ref, c, slots):
        return ref[c].at[slots] if isinstance(ref, tuple) else ref.at[c, slots]

    def send_part(source, target, sends, recvs, g, i, c, sign):
        k = bases[g] + i * capacity
        launch(piece(source, c, pl.ds(k, capacity)), piece(target, c, pl.ds(k, capacity)),
               sends.at[g], recvs.at[g, c], route(groups[g][i], sign))

    def await_group(source, target, recvs, g, c):
        many = pl.ds(bases[g] + capacity, (len(groups[g]) - 1) * capacity)
        pltpu.make_async_copy(piece(source, c, many), piece(target, c, many), recvs.at[g, c]).wait()

    def pick(g, i):
        for s in range(capacity):
            k = bases[g] + i * capacity + s
            n = jnp.clip(src_ref[k, 0], 0, total - 1)
            for c in range(chunks):
                value = made[n, c * rows:(c + 1) * rows, :]
                if i or (g == 3 and c < raw_out):
                    sent[c, k] = value
                if not i:
                    if g == 3 and c < raw_out:
                        @pl.when(outer)
                        def _():
                            came[c, k] = value
                    else:
                        came[c, k] = value

    def send_far(c):
        @pl.when(inner)
        def _():
            for r in (2, 1, 0):
                for d in reversed(range(ly)):
                    k = pl.ds(bases[3] + (r * ly + d) * capacity, capacity)
                    launch(sent.at[c, k], came.at[c, k], f_send, f_recv.at[r, c], at(0, steps[d], 2))

        @pl.when(outer)
        def _():
            for g, i in wide_parts:
                k = pl.ds(bases[g] + i * capacity, capacity)
                launch(sent.at[c, k], came.at[c, k], f_send, a_recv.at[g, c], route(groups[g][i], 1))

    near = [(g, i) for g in (2, 1, 0) for i in range(ly, 2 * ly)]
    wide_parts = [(3, i) for i in reversed(range(1, 3 * ly))]
    beside = [(g, i) for g in (2, 1, 0) for i in range(1, ly)]

    def send_near(c):
        for g, i in near:
            send_part(sent, came, a_send, a_recv, g, i, c, 1)

    for g, i in near:
        pick(g, i)
        send_part(sent, came, a_send, a_recv, g, i, 0, 1)
    for g, i in wide_parts + [(3, 0)]:
        pick(g, i)
    if raw_out:
        send_far(0)
    else:
        for g, i in wide_parts:
            send_part(sent, came, a_send, a_recv, g, i, 0, 1)
    for g, i in beside:
        pick(g, i)
        send_part(sent, came, a_send, a_recv, g, i, 0, 1)
    for g in range(3):
        pick(g, 0)
    ahead = max(1, chunks // 2)
    for c in range(1, chunks):
        if c < ahead:
            send_near(c)
        if c < raw_out:
            send_far(c)
        for g, i in ([] if c < raw_out else wide_parts) + beside:
            send_part(sent, came, a_send, a_recv, g, i, c, 1)

    def where_of(g, j):
        row = wide[j:j + 1, :] if g == 3 else tgt[g, j:j + 1, :]
        return jnp.broadcast_to(row, (8, lanes))

    def reduce(g, c, added, out):
        await_group(sent, came, a_recv, g, c)
        for r in range(rows // 8):
            at_rows = pl.ds(r * 8, 8)
            sums = [None] * OWNB
            for t in range(OWNB):
                for ref in added:
                    value = ref[c, t, at_rows, :]
                    sums[t] = value if sums[t] is None else sums[t] + value
            for j in range(len(groups[g]) * capacity):
                value = came[c, bases[g] + j, at_rows, :]
                where = where_of(g, j)
                for t in range(OWNB):
                    term = jnp.where(where == t, value, 0.0)
                    sums[t] = term if sums[t] is None else sums[t] + term
            for t in range(OWNB):
                out[c, t, at_rows, :] = sums[t]

    def add_far(g, c, out):
        pltpu.make_async_copy(sent.at[c, far_slots(g)], came.at[c, far_slots(g)], f_recv.at[g, c]).wait()
        for r in range(rows // 8):
            at_rows = pl.ds(r * 8, 8)
            sums = [out[c, t, at_rows, :] for t in range(OWNB)]
            for j in range(ly * capacity):
                value = came[c, bases[3] + g * ly * capacity + j, at_rows, :]
                where = where_of(g, 2 * ly * capacity + j)
                for t in range(OWNB):
                    sums[t] = sums[t] + jnp.where(where == t, value, 0.0)
            for t in range(OWNB):
                out[c, t, at_rows, :] = sums[t]

    def sum_role(g, c, added, out):
        reduce(g, c, added, out)
        if c < raw_out:
            @pl.when(inner)
            def _():
                add_far(g, c, out)

    def answer_far(g, c, held):
        for r in range(rows // 8):
            at_rows = pl.ds(r * 8, 8)
            values = [held[c, t, at_rows, :] for t in range(OWNB)]
            for j in range(ly * capacity):
                where = where_of(g, 2 * ly * capacity + j)
                out = values[0]
                for t in range(1, OWNB):
                    out = jnp.where(where == t, values[t], out)
                ans[c, bases[3] + g * ly * capacity + j, at_rows, :] = out
        for d in reversed(range(ly)):
            k = pl.ds(bases[3] + (g * ly + d) * capacity, capacity)
            launch(ans.at[c, k], back[c].at[k], e_send, e_recv.at[c], at(0, -steps[d], 2))

    def answer(g, c, held):
        if g < 3 and c >= raw_back:
            answer_part(g, c, held)

            @pl.when(inner)
            def _():
                answer_far(g, c, held)
        elif g == 3 and c >= raw_back:
            @pl.when(outer)
            def _():
                answer_part(g, c, held)
        else:
            answer_part(g, c, held)

    def answer_part(g, c, held):
        for r in range(rows // 8):
            at_rows = pl.ds(r * 8, 8)
            values = [held[c, t, at_rows, :] for t in range(OWNB)]
            for j in range(len(groups[g]) * capacity):
                where = where_of(g, j)
                out = values[0]
                for t in range(1, OWNB):
                    out = jnp.where(where == t, values[t], out)
                into = ans.at[c] if j >= capacity else back[c]
                into[bases[g] + j, at_rows, :] = out
        for i in reversed(range(1, len(groups[g]))):
            send_part(ans, back, b_send, b_recv, g, i, c, -1)

    outs = ((pd, ry, near_y), (px, rx, near_x), (wp, rw, far_z),
            (own, g1, near_x), (g1, g2, near_y), (own, w1, far_z))

    straight_out, straight_back = chunks - min(STRAIGHT_OUT, chunks), chunks - min(STRAIGHT_BACK, chunks)

    def pass_on(kind, c):
        source, target, device = outs[kind]
        if kind == 0 and c >= straight_out:
            device = corner
        if kind == 4 and c >= straight_back:
            source, device = own, corner
        launch(source.at[c], target.at[c], out_send.at[kind], out_recv.at[kind, c], device)

    def await_out(kind, c):
        source, target, _ = outs[kind]
        pltpu.make_async_copy(source.at[c], target.at[c], out_recv.at[kind, c]).wait()

    def sum_proxied(c):
        if c == 0:
            t_copies[0].wait_recv()

        def proxy():
            reduce(3, c, [], wp)
            pass_on(2, c)

        if c < raw_out:
            pl.when(outer)(proxy)
        else:
            proxy()
        if c + ahead < chunks:
            send_near(c + ahead)

    def sum_corner(c):
        if c == 0:
            t_copies[2].wait_recv()
        sum_role(2, c, [], pd)
        pass_on(0, c)

    def sum_near(c):
        if c == 0:
            t_copies[1].wait_recv()
        if c < straight_out:
            await_out(0, c)
        sum_role(1, c, [ry] if c < straight_out else [], px)
        pass_on(1, c)

    def sum_own(c):
        await_out(1, c)
        added = [rx]
        if c >= straight_out:
            await_out(0, c)
            added = [rx, ry]
        if c < raw_out:
            sum_role(0, c, added, own)

            @pl.when(outer)
            def _():
                await_out(2, c)
                own[c] = own[c] + rw[c]
        else:
            await_out(2, c)
            reduce(0, c, added + [rw], own)
        if c >= raw_back:
            pl.when(outer)(lambda: pass_on(5, c))
        else:
            pass_on(5, c)
        pass_on(3, c)
        if c >= straight_back:
            pass_on(4, c)
        answer(0, c, own)
        for t in range(OWNB):
            owned_ref[t, pl.ds(c * rows, rows), :] = own[c, t]

    def back_near(c):
        await_out(3, c)
        if c < straight_back:
            pass_on(4, c)
        answer(1, c, g1)

    def back_proxied(c):
        if c >= raw_back:
            @pl.when(outer)
            def _():
                await_out(5, c)
                answer_part(3, c, w1)
        else:
            await_out(5, c)
            answer_part(3, c, w1)

    def back_corner(c):
        await_out(4, c)
        answer(2, c, g2)

    def finish(c):
        for g in range(3):
            await_group(ans, back, b_recv, g, c)
        if c >= raw_back:
            pl.when(outer)(lambda: await_group(ans, back, b_recv, 3, c))

            @pl.when(inner)
            def _():
                pltpu.make_async_copy(ans.at[c, every_far], back[c].at[every_far], e_recv.at[c]).wait()
        else:
            await_group(ans, back, b_recv, 3, c)

        def place(p, carry):
            for b in range(block_count):
                comb_ref[p * block_count + b, pl.ds(c * rows, rows), :] = back[c][jnp.clip(key_ref[p, b], 0, came.shape[1] - 1)]
            return carry

        lax.fori_loop(0, patch_count, place, 0)

    def drain(ref, low, high, slots, sem):
        if high > low:
            view = ref.at[pl.ds(low, high - low)] if slots is None else ref.at[pl.ds(low, high - low), slots]
            pltpu.make_async_copy(view, view, sem).wait()

    def drain_sums():
        for copy in t_copies:
            copy.wait_send()
        for g, parts in enumerate(groups):
            many = pl.ds(bases[g] + capacity, (len(parts) - 1) * capacity)
            drain(sent, raw_out if g == 3 else 0, chunks, many, a_send.at[g])
        pl.when(inner)(lambda: drain(sent, 0, raw_out, every_far, f_send))
        pl.when(outer)(lambda: drain(sent, 0, raw_out, many, f_send))
        for kind, (source, _, _) in enumerate(outs):
            if kind in (2, 5):
                low, high = (raw_out, chunks) if kind == 2 else (0, raw_back)
                pl.when(inner)(lambda: drain(source, low, high, None, out_send.at[kind]))
                pl.when(outer)(lambda: drain(source, 0, chunks, None, out_send.at[kind]))
            else:
                drain(source, 0, chunks, None, out_send.at[kind])

    plan = [
        (sum_corner, 9.5, 2.8), (sum_proxied, 9.8, 2.1), (sum_near, 13.2, 2.8), (sum_own, 17.0, 3.0),
        (back_near, 20.6, 3.0), (back_proxied, 26.0, 2.1), (back_corner, 24.2, 3.0), (finish, 37.0, 1.0),
    ]
    timed = [(start + every * 4.0 / chunks * c, i, c) for i, (_, start, every) in enumerate(plan) for c in range(chunks)]
    early = {}
    for c in range(chunks):
        out, back_ = c >= straight_out, c >= straight_back
        early[2, c] = EARLY_N if out else 0.0
        early[3, c] = EARLY_O if out else 0.0
        early[4, c] = early[3, c]
        early[6, c] = early[3, c] + (EARLY_C if back_ else 0.0)
    timed = [(when - early.get((i, c), 0.0), i, c) for when, i, c in timed]
    for _, i, c in sorted(timed):
        if (i, c) == (len(plan) - 1, chunks - 1):
            drain_sums()
        plan[i][0](c)

    def drain(ref, low, high, slots, sem):
        if high > low:
            view = ref.at[pl.ds(low, high - low)] if slots is None else ref.at[pl.ds(low, high - low), slots]
            pltpu.make_async_copy(view, view, sem).wait()

    for g, parts in enumerate(groups):
        many = pl.ds(bases[g] + capacity, (len(parts) - 1) * capacity)
        if g < 3:
            drain(ans, 0, chunks, many, b_send.at[g])
        else:
            @pl.when(inner)
            def _():
                drain(ans, 0, raw_back, many, b_send.at[3])
                drain(ans, raw_back, chunks, every_far, e_send)

            @pl.when(outer)
            def _():
                drain(ans, 0, chunks, many, b_send.at[3])


def store_kernel(owned_ref, comb_ref, owned_hbm, comb_hbm, sem):
    copies = [
        pltpu.make_async_copy(comb_ref, comb_hbm, sem.at[0]),
        pltpu.make_async_copy(owned_ref, owned_hbm, sem.at[1])]
    for copy in copies:
        copy.start()
    for copy in copies:
        copy.wait()


def on_device(star_residual, patch_inverse, block_owner, block_slot, recv_target):
    nx, ny, nz = lax.axis_size("gx"), lax.axis_size("gy"), lax.axis_size("gz")
    patch_count, rhs_count, patch_order = star_residual.shape
    block_count = block_owner.shape[1]
    width = patch_order // block_count
    capacity = recv_target.shape[2]
    total = patch_count * block_count
    ly = len(offsets(ny))
    slots = 9 * ly * capacity
    tall = -(-slots // 8) * 8
    chunks = CHUNKS
    rows = rhs_count // chunks
    hbm = pl.BlockSpec(memory_space=pltpu.HBM)
    vmem = pl.BlockSpec(memory_space=pltpu.VMEM)
    anywhere = pl.BlockSpec(memory_space=pl.ANY)
    f32, i32 = jnp.float32, jnp.int32
    slotted = pltpu.VMEM((chunks, slots, rows, width), f32)
    targeted = pltpu.VMEM((chunks, OWNB, rows, width), f32)
    table = pltpu.VMEM((3, 3 * ly * capacity, width), i32)
    wide = pltpu.VMEM((3 * ly * capacity, width), i32)
    dma = pltpu.SemaphoreType.DMA
    limit = VMEM_BYTES - SPARE - (OWNB + total) * rhs_count * width * 4
    owned, comb = pl.pallas_call(
        functools.partial(kernel, (nx, ny, nz, chunks, capacity)),
        out_shape=(
            pltpu.VMEM((OWNB, rhs_count, width), f32),
            pltpu.VMEM((total, rhs_count, width), f32),
        ),
        in_specs=[hbm] * 5,
        out_specs=(vmem, vmem),
        scratch_shapes=[
            pltpu.VMEM(block_owner.shape, i32),
            pltpu.VMEM(block_slot.shape, i32),
            pltpu.SMEM((1, capacity, recv_target.shape[1]), i32),
            pltpu.VMEM((8, 128), i32),
            pltpu.VMEM((tall, 128), i32),
            pltpu.SMEM((8, 128), i32),
            pltpu.SMEM((tall, 128), i32),
            pltpu.VMEM(star_residual.shape, star_residual.dtype),
            pltpu.VMEM(patch_inverse.shape, patch_inverse.dtype),
            pltpu.VMEM((total, rhs_count, width), f32),
            slotted, slotted,
            table, table, wide, wide,
            targeted, targeted, targeted, targeted, targeted, targeted, targeted, targeted, targeted, targeted,
            slotted,
            dma((3,)), dma((patch_count + 2,)), dma((3,)), dma((3,)),
            dma((4,)), dma((4, chunks)), dma((4,)), dma((4, chunks)),
            dma((6,)), dma((6, chunks)),
            dma, dma((3, chunks)), dma, dma((chunks,)),
        ] + [pltpu.VMEM((slots, rows, width), f32)] * chunks,
        compiler_params=pltpu.CompilerParams(
            collective_id=0, has_side_effects=True, vmem_limit_bytes=limit),
    )(block_owner, block_slot, recv_target.transpose(0, 2, 1), star_residual, patch_inverse)
    owned, comb = pl.pallas_call(
        store_kernel,
        out_shape=(
            jax.ShapeDtypeStruct((OWNB, rhs_count, width), f32),
            jax.ShapeDtypeStruct((total, rhs_count, width), f32),
        ),
        in_specs=[anywhere, anywhere],
        out_specs=(anywhere, anywhere),
        scratch_shapes=[dma((2,))],
        compiler_params=pltpu.CompilerParams(vmem_limit_bytes=1024 * 1024),
    )(owned, comb)
    return owned, comb.reshape(patch_count, block_count, rhs_count, width)


def solution(mesh):
    placed = (
        P(("gx", "gy", "gz"), None, None),
        P(("gx", "gy", "gz"), None, None),
        P(("gx", "gy", "gz"), None),
        P(("gx", "gy", "gz"), None),
        P(("gx", "gy", "gz"), None, None),
    )
    return jax.shard_map(
        on_device,
        mesh=mesh,
        in_specs=placed,
        out_specs=(P(("gx", "gy", "gz"), None, None), P(("gx", "gy", "gz"), None, None, None)),
        check_vma=False,
    )
```

```python
import functools

import jax
import jax.numpy as jnp
from jax import lax
from jax.experimental import pallas as pl
from jax.experimental.pallas import tpu as pltpu
from jax.sharding import PartitionSpec as P

OWNB = 8
CHUNKS = 4
EARLY_N = 3.5
EARLY_O = 2.5
EARLY_C = 3.0
RAW_OUT = 2
RAW_BACK = 2
STRAIGHT_OUT = 1
STRAIGHT_BACK = 1
VMEM_BYTES = 67043328
SPARE = 131072
MESH = pl.DeviceIdType.MESH


def offsets(extent):
    return [0, 1, -1][: min(extent, 3)]


def offset_index(far, near, extent):
    step = far - near
    distance = jnp.where(step < 0, step + extent, step)
    return jnp.where(distance <= 1, distance, 2)


def role_of(at, here):
    return jnp.where((at > 0) & (lax.rem(here, 2) == 1), 3 - at, at)


def partner(here, role, extent):
    step = 1 - 2 * (here % 2)
    return (here + (0, step, extent - step)[role]) % extent


def role_code(here, role):
    parity = here % 2
    return (1, 2 * parity, 2 - 2 * parity)[role]


def kernel(cfg, owner_hbm, slot_hbm, table_hbm, star_hbm, inv_hbm, owned_ref, comb_ref,
           owner_ref, slot_ref, table_ref, key_out, src_out, key_ref, src_ref,
           star, inv, made, sent, came, tgt_out, tgt, wide_out, wide,
           pd, px, wp, ry, rx, rw, own, g1, g2, w1, ans,
           index_sem, load_sem, t_send, t_recv, a_send, a_recv, b_send, b_recv, out_send, out_recv,
           f_send, f_recv, e_send, e_recv, *back):
    nx, ny, nz, chunks, capacity = cfg
    gx, gy, gz = lax.axis_index("gx"), lax.axis_index("gy"), lax.axis_index("gz")
    patch_count, block_count = owner_hbm.shape
    total = patch_count * block_count
    rows, lanes = came.shape[2], came.shape[3]
    steps = offsets(ny)
    ly = len(steps)

    def at(role_x, dy, role_z):
        return (partner(gx, role_x, nx), (gy + dy + ny) % ny, partner(gz, role_z, nz))

    near_x, corner, far_z = at(1, 0, 0), at(2, 0, 0), at(0, 0, 2)
    near_y = ((gx + nx // 2) % nx, gy, gz)

    groups = [[(rz, d, r) for rz in (0, 1) for d in range(ly)] for r in range(3)]
    groups.append([(2, d, r) for r in range(3) for d in range(ly)])
    bases = [2 * ly * r * capacity for r in range(4)]
    raw_out, raw_back = min(RAW_OUT, chunks), chunks - min(RAW_BACK, chunks)
    inner = (gz > 0) & (gz < nz - 1)
    outer = jnp.logical_not(inner)

    def far_slots(r):
        return pl.ds(bases[3] + r * ly * capacity, ly * capacity)

    every_far = pl.ds(bases[3], 3 * ly * capacity)

    def route(part, sign):
        rz, d, r = part
        dy = sign * steps[d]
        return at(r, dy, 0) if rz == 2 else at(0, dy, rz)

    indices = [
        pltpu.make_async_copy(source, target, index_sem.at[i])
        for i, (source, target) in enumerate(
            ((owner_hbm, owner_ref), (slot_hbm, slot_ref), (table_hbm, table_ref)))]
    half = block_count // 2 * lanes
    loads = [pltpu.make_async_copy(star_hbm, star, load_sem.at[patch_count])]
    spans = [(0, 0, half), (0, half, block_count * lanes)]
    spans += [(p, 0, block_count * lanes) for p in range(1, patch_count)]
    for i, (p, low, high) in enumerate(spans):
        span = pl.ds(low, high - low)
        sem = load_sem.at[p if i else patch_count + 1]
        loads.append(pltpu.make_async_copy(inv_hbm.at[p, span], inv.at[p, span], sem))
    for load in indices + loads[:3]:
        load.start()

    barrier = pltpu.get_barrier_semaphore()
    greeted = [at(0, dy, rz) for dy in steps for rz in (0, 1, 2) if dy or rz]
    greeted += [at(r, dy, 0) for dy in steps for r in (1, 2)] + [near_y]
    for device in greeted:
        pl.semaphore_signal(barrier, inc=1, device_id=device, device_id_type=MESH)

    for load in indices:
        load.wait()
    for load in loads[3:]:
        load.start()

    def multiply(i):
        p, low, high = spans[i]
        loads[1 + i].wait()
        block = lax.dot_general(
            star[p], inv[p, low:high, :], (((1,), (1,)), ((), ())), preferred_element_type=jnp.float32)
        for b in range((high - low) // lanes):
            made[p * block_count + low // lanes + b] = block[:, b * lanes:(b + 1) * lanes]

    loads[0].wait()
    multiply(0)
    multiply(1)

    owner = owner_ref[...]
    owner_x = sum(((owner >= i * ny * nz).astype(jnp.int32) for i in range(1, nx)), jnp.zeros_like(owner))
    owner = owner - owner_x * (ny * nz)
    owner_y = sum(((owner >= i * nz).astype(jnp.int32) for i in range(1, ny)), jnp.zeros_like(owner))
    role_x = role_of(offset_index(owner_x, gx, nx), gx)
    at_y = offset_index(owner_y, gy, ny)
    role_z = role_of(offset_index(owner - owner_y * nz, gz, nz), gz)
    where = jnp.where(role_z == 2, 6 * ly + role_x * ly + at_y, (2 * role_x + role_z) * ly + at_y)
    key = where * capacity + slot_ref[...]
    key_out[0:patch_count, 0:block_count] = key
    tall = src_out.shape[0]
    number = lax.broadcasted_iota(jnp.int32, (tall, block_count), 0)
    block = lax.broadcasted_iota(jnp.int32, (tall, block_count), 1)
    found = jnp.zeros((tall, block_count), jnp.int32)
    for p in range(patch_count):
        hit = jnp.broadcast_to(key[p:p + 1, :], (tall, block_count)) == number
        found = jnp.maximum(found, jnp.where(hit, block + p * block_count, 0))
    src_out[...] = jnp.broadcast_to(
        jnp.max(found, axis=1, keepdims=True), src_out.shape)
    scalars = [
        pltpu.make_async_copy(key_out, key_ref, index_sem.at[0]),
        pltpu.make_async_copy(src_out, src_ref, index_sem.at[1])]
    for load in scalars:
        load.start()

    def entry(role_x, dy, role_z, s):
        code = 9 * role_code(gx, role_x) + 3 * (dy + 1) + role_code(gz, role_z)
        return jnp.full((1, lanes), table_ref[0, s, code], jnp.int32)

    for r in range(3):
        for rz in range(3):
            for d, dy in enumerate(steps):
                for s in range(capacity):
                    row = entry(r, dy, rz, s)
                    j = (rz * ly + d) * capacity + s
                    held = tgt_out if r else tgt
                    held[r, j:j + 1, :] = row
                    if rz == 2:
                        j = (r * ly + d) * capacity + s
                        wide_out[j:j + 1, :] = row

    for i in range(2, len(spans) - 1):
        multiply(i)

    pl.semaphore_wait(barrier, len(greeted))

    def launch(source, target, send_sem, recv_sem, device):
        copy = pltpu.make_async_remote_copy(
            src_ref=source, dst_ref=target, send_sem=send_sem, recv_sem=recv_sem,
            device_id=device, device_id_type=MESH)
        copy.start()
        return copy

    t_copies = [
        launch(wide_out, wide, t_send.at[2], t_recv.at[2], far_z),
        launch(tgt_out.at[1], tgt.at[1], t_send.at[0], t_recv.at[0], near_x),
        launch(tgt_out.at[2], tgt.at[2], t_send.at[1], t_recv.at[1], corner),
    ]

    multiply(len(spans) - 1)
    for load in scalars:
        load.wait()

    def piece(ref, c, slots):
        return ref[c].at[slots] if isinstance(ref, tuple) else ref.at[c, slots]

    def send_part(source, target, sends, recvs, g, i, c, sign):
        k = bases[g] + i * capacity
        launch(piece(source, c, pl.ds(k, capacity)), piece(target, c, pl.ds(k, capacity)),
               sends.at[g], recvs.at[g, c], route(groups[g][i], sign))

    def await_group(source, target, recvs, g, c):
        many = pl.ds(bases[g] + capacity, (len(groups[g]) - 1) * capacity)
        pltpu.make_async_copy(piece(source, c, many), piece(target, c, many), recvs.at[g, c]).wait()

    def pick(g, i):
        for s in range(capacity):
            k = bases[g] + i * capacity + s
            n = jnp.clip(src_ref[k, 0], 0, total - 1)
            for c in range(chunks):
                value = made[n, c * rows:(c + 1) * rows, :]
                if i or (g == 3 and c < raw_out):
                    sent[c, k] = value
                if not i:
                    if g == 3 and c < raw_out:
                        @pl.when(outer)
                        def _():
                            came[c, k] = value
                    else:
                        came[c, k] = value

    def send_far(c):
        @pl.when(inner)
        def _():
            for r in (2, 1, 0):
                for d in reversed(range(ly)):
                    k = pl.ds(bases[3] + (r * ly + d) * capacity, capacity)
                    launch(sent.at[c, k], came.at[c, k], f_send, f_recv.at[r, c], at(0, steps[d], 2))

        @pl.when(outer)
        def _():
            for g, i in wide_parts:
                k = pl.ds(bases[g] + i * capacity, capacity)
                launch(sent.at[c, k], came.at[c, k], f_send, a_recv.at[g, c], route(groups[g][i], 1))

    near = [(g, i) for g in (2, 1, 0) for i in range(ly, 2 * ly)]
    wide_parts = [(3, i) for i in reversed(range(1, 3 * ly))]
    beside = [(g, i) for g in (2, 1, 0) for i in range(1, ly)]

    def send_near(c):
        for g, i in near:
            send_part(sent, came, a_send, a_recv, g, i, c, 1)

    for g, i in near:
        pick(g, i)
        send_part(sent, came, a_send, a_recv, g, i, 0, 1)
    for g, i in wide_parts + [(3, 0)]:
        pick(g, i)
    if raw_out:
        send_far(0)
    else:
        for g, i in wide_parts:
            send_part(sent, came, a_send, a_recv, g, i, 0, 1)
    for g, i in beside:
        pick(g, i)
        send_part(sent, came, a_send, a_recv, g, i, 0, 1)
    for g in range(3):
        pick(g, 0)
    ahead = max(1, chunks // 2)
    for c in range(1, chunks):
        if c < ahead:
            send_near(c)
        if c < raw_out:
            send_far(c)
        for g, i in ([] if c < raw_out else wide_parts) + beside:
            send_part(sent, came, a_send, a_recv, g, i, c, 1)

    def where_of(g, j):
        row = wide[j:j + 1, :] if g == 3 else tgt[g, j:j + 1, :]
        return jnp.broadcast_to(row, (8, lanes))

    def reduce(g, c, added, out):
        await_group(sent, came, a_recv, g, c)
        for r in range(rows // 8):
            at_rows = pl.ds(r * 8, 8)
            sums = [None] * OWNB
            for t in range(OWNB):
                for ref in added:
                    value = ref[c, t, at_rows, :]
                    sums[t] = value if sums[t] is None else sums[t] + value
            for j in range(len(groups[g]) * capacity):
                value = came[c, bases[g] + j, at_rows, :]
                where = where_of(g, j)
                for t in range(OWNB):
                    term = jnp.where(where == t, value, 0.0)
                    sums[t] = term if sums[t] is None else sums[t] + term
            for t in range(OWNB):
                out[c, t, at_rows, :] = sums[t]

    def add_far(g, c, out):
        pltpu.make_async_copy(sent.at[c, far_slots(g)], came.at[c, far_slots(g)], f_recv.at[g, c]).wait()
        for r in range(rows // 8):
            at_rows = pl.ds(r * 8, 8)
            sums = [out[c, t, at_rows, :] for t in range(OWNB)]
            for j in range(ly * capacity):
                value = came[c, bases[3] + g * ly * capacity + j, at_rows, :]
                where = where_of(g, 2 * ly * capacity + j)
                for t in range(OWNB):
                    sums[t] = sums[t] + jnp.where(where == t, value, 0.0)
            for t in range(OWNB):
                out[c, t, at_rows, :] = sums[t]

    def sum_role(g, c, added, out):
        reduce(g, c, added, out)
        if c < raw_out:
            @pl.when(inner)
            def _():
                add_far(g, c, out)

    def answer_far(g, c, held):
        for r in range(rows // 8):
            at_rows = pl.ds(r * 8, 8)
            values = [held[c, t, at_rows, :] for t in range(OWNB)]
            for j in range(ly * capacity):
                where = where_of(g, 2 * ly * capacity + j)
                out = values[0]
                for t in range(1, OWNB):
                    out = jnp.where(where == t, values[t], out)
                ans[c, bases[3] + g * ly * capacity + j, at_rows, :] = out
        for d in reversed(range(ly)):
            k = pl.ds(bases[3] + (g * ly + d) * capacity, capacity)
            launch(ans.at[c, k], back[c].at[k], e_send, e_recv.at[c], at(0, -steps[d], 2))

    def answer(g, c, held):
        if g < 3 and c >= raw_back:
            answer_part(g, c, held)

            @pl.when(inner)
            def _():
                answer_far(g, c, held)
        elif g == 3 and c >= raw_back:
            @pl.when(outer)
            def _():
                answer_part(g, c, held)
        else:
            answer_part(g, c, held)

    def answer_part(g, c, held):
        for r in range(rows // 8):
            at_rows = pl.ds(r * 8, 8)
            values = [held[c, t, at_rows, :] for t in range(OWNB)]
            for j in range(len(groups[g]) * capacity):
                where = where_of(g, j)
                out = values[0]
                for t in range(1, OWNB):
                    out = jnp.where(where == t, values[t], out)
                into = ans.at[c] if j >= capacity else back[c]
                into[bases[g] + j, at_rows, :] = out
        for i in reversed(range(1, len(groups[g]))):
            send_part(ans, back, b_send, b_recv, g, i, c, -1)

    outs = ((pd, ry, near_y), (px, rx, near_x), (wp, rw, far_z),
            (own, g1, near_x), (g1, g2, near_y), (own, w1, far_z))

    straight_out, straight_back = chunks - min(STRAIGHT_OUT, chunks), chunks - min(STRAIGHT_BACK, chunks)

    def pass_on(kind, c):
        source, target, device = outs[kind]
        if kind == 0 and c >= straight_out:
            device = corner
        if kind == 4 and c >= straight_back:
            source, device = own, corner
        launch(source.at[c], target.at[c], out_send.at[kind], out_recv.at[kind, c], device)

    def await_out(kind, c):
        source, target, _ = outs[kind]
        pltpu.make_async_copy(source.at[c], target.at[c], out_recv.at[kind, c]).wait()

    def sum_proxied(c):
        if c == 0:
            t_copies[0].wait_recv()

        def proxy():
            reduce(3, c, [], wp)
            pass_on(2, c)

        if c < raw_out:
            pl.when(outer)(proxy)
        else:
            proxy()
        if c + ahead < chunks:
            send_near(c + ahead)

    def sum_corner(c):
        if c == 0:
            t_copies[2].wait_recv()
        sum_role(2, c, [], pd)
        pass_on(0, c)

    def sum_near(c):
        if c == 0:
            t_copies[1].wait_recv()
        if c < straight_out:
            await_out(0, c)
        sum_role(1, c, [ry] if c < straight_out else [], px)
        pass_on(1, c)

    def sum_own(c):
        await_out(1, c)
        added = [rx]
        if c >= straight_out:
            await_out(0, c)
            added = [rx, ry]
        if c < raw_out:
            sum_role(0, c, added, own)

            @pl.when(outer)
            def _():
                await_out(2, c)
                own[c] = own[c] + rw[c]
        else:
            await_out(2, c)
            reduce(0, c, added + [rw], own)
        if c >= raw_back:
            pl.when(outer)(lambda: pass_on(5, c))
        else:
            pass_on(5, c)
        pass_on(3, c)
        if c >= straight_back:
            pass_on(4, c)
        answer(0, c, own)
        for t in range(OWNB):
            owned_ref[t, pl.ds(c * rows, rows), :] = own[c, t]

    def back_near(c):
        await_out(3, c)
        if c < straight_back:
            pass_on(4, c)
        answer(1, c, g1)

    def back_proxied(c):
        if c >= raw_back:
            @pl.when(outer)
            def _():
                await_out(5, c)
                answer_part(3, c, w1)
        else:
            await_out(5, c)
            answer_part(3, c, w1)

    def back_corner(c):
        await_out(4, c)
        answer(2, c, g2)

    def finish(c):
        for g in range(3):
            await_group(ans, back, b_recv, g, c)
        if c >= raw_back:
            pl.when(outer)(lambda: await_group(ans, back, b_recv, 3, c))

            @pl.when(inner)
            def _():
                pltpu.make_async_copy(ans.at[c, every_far], back[c].at[every_far], e_recv.at[c]).wait()
        else:
            await_group(ans, back, b_recv, 3, c)

        def place(p, carry):
            for b in range(block_count):
                comb_ref[p * block_count + b, pl.ds(c * rows, rows), :] = back[c][jnp.clip(key_ref[p, b], 0, came.shape[1] - 1)]
            return carry

        lax.fori_loop(0, patch_count, place, 0)

    def drain(ref, low, high, slots, sem):
        if high > low:
            view = ref.at[pl.ds(low, high - low)] if slots is None else ref.at[pl.ds(low, high - low), slots]
            pltpu.make_async_copy(view, view, sem).wait()

    def drain_sums():
        for copy in t_copies:
            copy.wait_send()
        for g, parts in enumerate(groups):
            many = pl.ds(bases[g] + capacity, (len(parts) - 1) * capacity)
            drain(sent, raw_out if g == 3 else 0, chunks, many, a_send.at[g])
        pl.when(inner)(lambda: drain(sent, 0, raw_out, every_far, f_send))
        pl.when(outer)(lambda: drain(sent, 0, raw_out, many, f_send))
        for kind, (source, _, _) in enumerate(outs):
            if kind in (2, 5):
                low, high = (raw_out, chunks) if kind == 2 else (0, raw_back)
                pl.when(inner)(lambda: drain(source, low, high, None, out_send.at[kind]))
                pl.when(outer)(lambda: drain(source, 0, chunks, None, out_send.at[kind]))
            else:
                drain(source, 0, chunks, None, out_send.at[kind])

    plan = [
        (sum_corner, 9.5, 2.8), (sum_proxied, 9.8, 2.1), (sum_near, 13.2, 2.8), (sum_own, 17.0, 3.0),
        (back_near, 20.6, 3.0), (back_proxied, 25.5, 1.9), (back_corner, 24.2, 3.0), (finish, 37.0, 1.0),
    ]
    timed = [(start + every * 4.0 / chunks * c, i, c) for i, (_, start, every) in enumerate(plan) for c in range(chunks)]
    early = {}
    for c in range(chunks):
        out, back_ = c >= straight_out, c >= straight_back
        early[2, c] = EARLY_N if out else 0.0
        early[3, c] = EARLY_O if out else 0.0
        early[4, c] = early[3, c]
        early[6, c] = early[3, c] + (EARLY_C if back_ else 0.0)
    timed = [(when - early.get((i, c), 0.0), i, c) for when, i, c in timed]
    for _, i, c in sorted(timed):
        if (i, c) == (len(plan) - 1, chunks - 1):
            drain_sums()
        plan[i][0](c)

    def drain(ref, low, high, slots, sem):
        if high > low:
            view = ref.at[pl.ds(low, high - low)] if slots is None else ref.at[pl.ds(low, high - low), slots]
            pltpu.make_async_copy(view, view, sem).wait()

    for g, parts in enumerate(groups):
        many = pl.ds(bases[g] + capacity, (len(parts) - 1) * capacity)
        if g < 3:
            drain(ans, 0, chunks, many, b_send.at[g])
        else:
            @pl.when(inner)
            def _():
                drain(ans, 0, raw_back, many, b_send.at[3])
                drain(ans, raw_back, chunks, every_far, e_send)

            @pl.when(outer)
            def _():
                drain(ans, 0, chunks, many, b_send.at[3])


def store_kernel(owned_ref, comb_ref, owned_hbm, comb_hbm, sem):
    copies = [
        pltpu.make_async_copy(comb_ref, comb_hbm, sem.at[0]),
        pltpu.make_async_copy(owned_ref, owned_hbm, sem.at[1])]
    for copy in copies:
        copy.start()
    for copy in copies:
        copy.wait()


def on_device(star_residual, patch_inverse, block_owner, block_slot, recv_target):
    nx, ny, nz = lax.axis_size("gx"), lax.axis_size("gy"), lax.axis_size("gz")
    patch_count, rhs_count, patch_order = star_residual.shape
    block_count = block_owner.shape[1]
    width = patch_order // block_count
    capacity = recv_target.shape[2]
    total = patch_count * block_count
    ly = len(offsets(ny))
    slots = 9 * ly * capacity
    tall = -(-slots // 8) * 8
    chunks = CHUNKS
    rows = rhs_count // chunks
    hbm = pl.BlockSpec(memory_space=pltpu.HBM)
    vmem = pl.BlockSpec(memory_space=pltpu.VMEM)
    anywhere = pl.BlockSpec(memory_space=pl.ANY)
    f32, i32 = jnp.float32, jnp.int32
    slotted = pltpu.VMEM((chunks, slots, rows, width), f32)
    targeted = pltpu.VMEM((chunks, OWNB, rows, width), f32)
    table = pltpu.VMEM((3, 3 * ly * capacity, width), i32)
    wide = pltpu.VMEM((3 * ly * capacity, width), i32)
    dma = pltpu.SemaphoreType.DMA
    limit = VMEM_BYTES - SPARE - (OWNB + total) * rhs_count * width * 4
    owned, comb = pl.pallas_call(
        functools.partial(kernel, (nx, ny, nz, chunks, capacity)),
        out_shape=(
            pltpu.VMEM((OWNB, rhs_count, width), f32),
            pltpu.VMEM((total, rhs_count, width), f32),
        ),
        in_specs=[hbm] * 5,
        out_specs=(vmem, vmem),
        scratch_shapes=[
            pltpu.VMEM(block_owner.shape, i32),
            pltpu.VMEM(block_slot.shape, i32),
            pltpu.SMEM((1, capacity, recv_target.shape[1]), i32),
            pltpu.VMEM((8, 128), i32),
            pltpu.VMEM((tall, 128), i32),
            pltpu.SMEM((8, 128), i32),
            pltpu.SMEM((tall, 128), i32),
            pltpu.VMEM(star_residual.shape, star_residual.dtype),
            pltpu.VMEM(patch_inverse.shape, patch_inverse.dtype),
            pltpu.VMEM((total, rhs_count, width), f32),
            slotted, slotted,
            table, table, wide, wide,
            targeted, targeted, targeted, targeted, targeted, targeted, targeted, targeted, targeted, targeted,
            slotted,
            dma((3,)), dma((patch_count + 2,)), dma((3,)), dma((3,)),
            dma((4,)), dma((4, chunks)), dma((4,)), dma((4, chunks)),
            dma((6,)), dma((6, chunks)),
            dma, dma((3, chunks)), dma, dma((chunks,)),
        ] + [pltpu.VMEM((slots, rows, width), f32)] * chunks,
        compiler_params=pltpu.CompilerParams(
            collective_id=0, has_side_effects=True, vmem_limit_bytes=limit),
    )(block_owner, block_slot, recv_target.transpose(0, 2, 1), star_residual, patch_inverse)
    owned, comb = pl.pallas_call(
        store_kernel,
        out_shape=(
            jax.ShapeDtypeStruct((OWNB, rhs_count, width), f32),
            jax.ShapeDtypeStruct((total, rhs_count, width), f32),
        ),
        in_specs=[anywhere, anywhere],
        out_specs=(anywhere, anywhere),
        scratch_shapes=[dma((2,))],
        compiler_params=pltpu.CompilerParams(vmem_limit_bytes=1024 * 1024),
    )(owned, comb)
    return owned, comb.reshape(patch_count, block_count, rhs_count, width)


def solution(mesh):
    placed = (
        P(("gx", "gy", "gz"), None, None),
        P(("gx", "gy", "gz"), None, None),
        P(("gx", "gy", "gz"), None),
        P(("gx", "gy", "gz"), None),
        P(("gx", "gy", "gz"), None, None),
    )
    return jax.shard_map(
        on_device,
        mesh=mesh,
        in_specs=placed,
        out_specs=(P(("gx", "gy", "gz"), None, None), P(("gx", "gy", "gz"), None, None, None)),
        check_vma=False,
    )
```
